32 devices in a mesh: graphs: 2 (over y), rows: 4 (over z), cols: 2 (over x), sub: 2 (over core).
Axes of the slice: x: 2, y: 2, z: 4, core: 2. Of those that a mesh axis runs over, the one named last changes fastest.
Arguments:
- current_block: float32 [16, 65536], P(None, ('graphs', 'rows', 'cols', 'sub')), parts along dimension 1, may hold values from -1200 to 1200, as said below
- previous_block: float32 [16, 65536], P(None, ('graphs', 'rows', 'cols', 'sub')), parts along dimension 1, may hold values from -1200 to 1200, as said below
- adjacency_tiles: float32 [1536, 128, 128], P(('graphs', 'rows', 'cols', 'sub')), parts along dimension 0, may hold values from -0.3125 to 0.3125
- tile_rows: int32 [1536], P(('graphs', 'rows', 'cols', 'sub')), parts along dimension 0, may hold values from 0 to 255, as said below
- tile_cols: int32 [1536], P(('graphs', 'rows', 'cols', 'sub')), parts along dimension 0, may hold values from 0 to 255, as said below
- tile_count: int32 [32], P(('graphs', 'rows', 'cols', 'sub')), parts along dimension 0, may hold values from 18 to 48, as said below
- locked: int32 [2], P('graphs'), parts along dimension 0, may hold values from 0 to 7
Outputs:
- w_basis: float32 [16, 65536], P(None, ('graphs', 'rows', 'cols', 'sub')), parts along dimension 1
- w_image: float32 [16, 65536], P(None, ('graphs', 'rows', 'cols', 'sub')), parts along dimension 1
- ritz_matrix: float32 [96, 48], P('graphs'), parts along dimension 0
The draws below stay inside these ranges and needn't reach their ends.
There are 2 independent parts, one for each index of `graphs`. The reference program is written for one: setup_inputs(seed, part) draws one part's arguments, and reference() takes and returns one part's arrays. A program takes and returns all parts, laid end to end along the dimension named above; each array names one. Nothing has to cross between parts.
Inputs may be any that keep to these rules, and one draw needn't show every extreme that they name: `current_block`: entries of order one to some hundreds. `previous_block`: entries of order one to some hundreds. Slots d * 48 to (d + 1) * 48 - 1 belong to device d and name its own tile rows d * 16 to (d + 1) * 16 - 1. The first 16 slots of a device name its tile rows in order, with tile_cols equal to tile_rows. Slots past the device's count name tile row d * 16 and carry no weight. `tile_cols`: A slot of device d names a tile column from d * 16 - 8 to (d + 1) * 16 + 7. Slot 16 of a device names a tile of the block before it and slot 17 one of the block after it, where such a block exists. A pair of tile row and tile column may stand in several slots; their tiles add. `tile_count`: in every draw some device has all 48 slots live.
All inputs are finite; a program needn't handle non-finite values.
Results may differ from the reference program's by a relative error of at most 0.000094.
Values sent between devices are 32-bit elements; how exact they have to be, the bound alone decides.
No kernel may reach another device: no remote copies, remote signals or barrier semaphores. Data moves between devices by JAX's collectives and lax.ppermute only.
A program may use at most 64 MiB of HBM per device.

```python
import jax
import jax.numpy as jnp
from jax import lax

K = 16
TILE_VERTICES = 128
DEVICE_SLOTS = 3
DEVS = 16
DEVICE_TILE_ROWS = 16
REACH = 8
MAXT_DEV = 48
NV = 32768
NT = 256
GRAPH_SLOTS = 768


def tile_arrangement(key):
    keys = jax.random.split(jax.random.fold_in(key, 11), 6)
    devices = jnp.arange(DEVS, dtype=jnp.int32)
    slot_indices = jnp.arange(MAXT_DEV, dtype=jnp.int32)[None, :]
    extra = jax.random.randint(keys[0], (DEVS,), 2, MAXT_DEV - DEVICE_TILE_ROWS + 1)
    fullest = jax.random.randint(keys[1], (), 0, DEVS)
    extra = jnp.where(devices == fullest, MAXT_DEV - DEVICE_TILE_ROWS, extra)
    counts = (DEVICE_TILE_ROWS + extra).astype(jnp.int32)
    row_offset = jax.random.randint(keys[2], (DEVS, MAXT_DEV), 0, DEVICE_TILE_ROWS)
    col_offset = jax.random.randint(keys[3], (DEVS, MAXT_DEV), -REACH, DEVICE_TILE_ROWS + REACH)
    left_offset = jax.random.randint(keys[4], (DEVS, MAXT_DEV), -REACH, 0)
    right_offset = DEVICE_TILE_ROWS + jax.random.randint(keys[5], (DEVS, MAXT_DEV), 0, REACH)
    col_offset = jnp.where(slot_indices == DEVICE_TILE_ROWS, left_offset, col_offset)
    col_offset = jnp.where(slot_indices == DEVICE_TILE_ROWS + 1, right_offset, col_offset)
    diagonal = slot_indices < DEVICE_TILE_ROWS
    row_offset = jnp.where(diagonal, slot_indices, row_offset)
    col_offset = jnp.where(diagonal, slot_indices, col_offset)
    padded = slot_indices >= counts[:, None]
    row_offset = jnp.where(padded, 0, row_offset)
    col_offset = jnp.where(padded, 0, col_offset)
    rows_out = devices[:, None] * DEVICE_TILE_ROWS + row_offset
    cols_out = devices[:, None] * DEVICE_TILE_ROWS + col_offset
    cols_out = jnp.where(cols_out < 0, cols_out + REACH, cols_out)
    cols_out = jnp.where(cols_out >= NT, cols_out - REACH, cols_out)
    return (rows_out.reshape(-1).astype(jnp.int32), cols_out.reshape(-1).astype(jnp.int32), counts)


def draw_tile_rows(key, part):
    return tile_arrangement(key)[0]


def draw_tile_cols(key, part):
    return tile_arrangement(key)[1]


def draw_tile_count(key, part):
    return tile_arrangement(key)[2]


def draw_locked(key, part):
    base = jax.random.randint(jax.random.fold_in(key, 53), (1,), 0, 7)
    return jnp.where(part % 2 == 1, 7, base).astype(jnp.int32)


def vector_draw(key):
    keys = jax.random.split(key, 4)
    where_along = jnp.arange(NV, dtype=jnp.float32) / NV
    rising = jnp.sqrt(1.0 + 2.0 * where_along)
    base = jax.random.truncated_normal(keys[0], -5.0, 5.0, (K, NV), jnp.float32)
    rough = 10.0 ** jax.random.uniform(keys[2], (NV,), jnp.float32)
    column_scale = 10.0 ** jax.random.uniform(keys[3], (K,), jnp.float32)
    return base * (rough * rising)[None, :] * column_scale[:, None]


def draw_current_block(key, part):
    return vector_draw(jax.random.fold_in(key, 21))


def draw_previous_block(key, part):
    return vector_draw(jax.random.fold_in(key, 37))


def shard_levels(rng, dims, cuts, smallest, high):
    loudness = 1.0
    for dim, blocks in cuts:
        draws = jax.random.uniform(jax.random.fold_in(jax.random.fold_in(rng, 6), dim), (blocks,), jnp.float32, smallest / len(cuts), high / len(cuts))
        loudness = loudness * jnp.repeat(jnp.exp(draws), dims[dim] // blocks).reshape((-1,) + (1,) * (len(dims) - 1 - dim))
    return loudness


def normal_values(rng, dims, spread, most, shards=(), kind=jnp.bfloat16):
    drawn = spread * jax.random.normal(rng, dims, jnp.float32)
    if shards:
        drawn = drawn * shard_levels(rng, dims, shards, -0.22, 0.18)
    return jnp.clip(drawn, -most, most).astype(kind)


def setup_inputs(seed: int = 0, part: int = 0) -> dict:
    splits = jax.random.split(jax.random.key(seed), 8)
    own_keys = jax.random.split(jax.random.fold_in(splits[7], part), 8)
    return {
        "current_block": draw_current_block(jax.random.fold_in(jax.random.fold_in(splits[7], part), 71), part),
        "previous_block": draw_previous_block(jax.random.fold_in(jax.random.fold_in(splits[7], part), 71), part),
        "adjacency_tiles": normal_values(own_keys[2], (GRAPH_SLOTS, TILE_VERTICES, TILE_VERTICES), (DEVICE_SLOTS * TILE_VERTICES) ** -0.5, 0.3125, ((0, 16),), jnp.float32),
        "tile_rows": draw_tile_rows(jax.random.fold_in(jax.random.fold_in(splits[7], part), 71), part),
        "tile_cols": draw_tile_cols(jax.random.fold_in(jax.random.fold_in(splits[7], part), 71), part),
        "tile_count": draw_tile_count(jax.random.fold_in(jax.random.fold_in(splits[7], part), 71), part),
        "locked": draw_locked(jax.random.fold_in(jax.random.fold_in(splits[7], part), 71), part),
    }


def apply_operator(vectors, adjacency_tiles, tile_rows, tile_cols, live_mask):
    channels = vectors.shape[0]
    column_blocks = vectors.reshape(channels, NT, TILE_VERTICES)
    gathered = jnp.take(column_blocks, tile_cols, axis=1)
    products = jnp.einsum('cta,tab->tcb', gathered, adjacency_tiles, precision=lax.Precision.HIGHEST)
    products = products * live_mask[:, None, None]
    summed = jax.ops.segment_sum(products, tile_rows, num_segments=NT)
    return vectors - jnp.transpose(summed, (1, 0, 2)).reshape(channels, NV)

def inner_products(left, right):
    return jnp.dot(left, right.T, precision=lax.Precision.HIGHEST)

def rayleigh_ritz(gram_b, gram_a):
    factor_b = jnp.linalg.cholesky(gram_b)
    symmetric = 0.5 * (gram_a + gram_a.T)
    halfway = lax.linalg.triangular_solve(factor_b, symmetric, left_side=True, lower=True)
    return lax.linalg.triangular_solve(factor_b, halfway.T, left_side=True, lower=True)

def reference(current_block, previous_block, adjacency_tiles, tile_rows, tile_cols, tile_count, locked):
    slot_indices = jnp.arange(GRAPH_SLOTS, dtype=jnp.int32)
    owners = slot_indices // MAXT_DEV
    live_mask = (slot_indices % MAXT_DEV < tile_count[owners]).astype(jnp.float32)
    stacked = jnp.concatenate([current_block, previous_block], axis=0)
    images = apply_operator(stacked, adjacency_tiles, tile_rows, tile_cols, live_mask)
    x_image = images[:K]
    p_image = images[K:]
    quotient = jnp.sum(current_block * x_image, axis=1) / (jnp.sum(current_block * current_block, axis=1) + 1e-06)
    frozen_rows = jnp.arange(K, dtype=jnp.int32) < locked[0]
    residual = jnp.where(frozen_rows[:, None], 0.0, x_image - quotient[:, None] * current_block)
    gram_w = inner_products(residual, residual) / NV + jnp.diag(frozen_rows.astype(jnp.float32))
    factor = jnp.linalg.cholesky(gram_w)
    w_basis = lax.linalg.triangular_solve(factor, residual, left_side=True, lower=True)
    w_image = apply_operator(w_basis, adjacency_tiles, tile_rows, tile_cols, live_mask)
    search = jnp.concatenate([current_block, w_basis, previous_block], axis=0)
    search_image = jnp.concatenate([x_image, w_image, p_image], axis=0)
    zero_rows = jnp.zeros((K,), jnp.float32)
    pad_diag = jnp.concatenate([zero_rows, frozen_rows.astype(jnp.float32), zero_rows])
    gram_b = inner_products(search, search) / NV + jnp.diag(pad_diag)
    gram_a = inner_products(search, search_image) / NV
    ritz_matrix = rayleigh_ritz(gram_b, gram_a)
    return (w_basis, w_image, ritz_matrix)
```

```python
import functools

import jax
import jax.numpy as jnp
from jax import lax
from jax.experimental import pallas as pl
from jax.experimental.pallas import tpu as pltpu
from jax.sharding import PartitionSpec as P

AXES = ("rows", "cols", "sub")
F32 = jnp.float32
BF16 = jnp.bfloat16
HIGHEST = lax.Precision.HIGHEST
LANES = 128
UNROLL = 8
VMEM = pl.BlockSpec(memory_space=pltpu.VMEM)
SMEM = pl.BlockSpec(memory_space=pltpu.SMEM)


def split3(x):
    a = x.astype(BF16)
    rest = x - a.astype(F32)
    b = rest.astype(BF16)
    c = (rest - b.astype(F32)).astype(BF16)
    return a, b, c


def store_parts(parts_ref, tile, at, height, values):
    channels = values.shape[0]
    for k, part in enumerate(split3(values)):
        parts_ref[tile, k * height + at : k * height + at + channels, :] = part


def load_span(parts_ref, at, height, left_ref, mid_ref, right_ref, tile):
    reach = left_ref.shape[1] // tile
    rows = mid_ref.shape[1] // tile
    for k in range(reach):
        cut = slice(k * tile, (k + 1) * tile)
        store_parts(parts_ref, k, at, height, left_ref[:, cut])
        store_parts(parts_ref, reach + rows + k, at, height, right_ref[:, cut])
    for k in range(rows):
        store_parts(parts_ref, reach + k, at, height, mid_ref[:, k * tile : (k + 1) * tile])


def tile_product(parts_ref, tiles_ref, t, col, height):
    lhs = parts_ref[col]
    t1, t2, t3 = split3(tiles_ref[t])
    y1 = jnp.dot(lhs, t1, preferred_element_type=F32)
    y2 = jnp.dot(lhs[: 2 * height], t2, preferred_element_type=F32)
    y3 = jnp.dot(lhs[:height], t3, preferred_element_type=F32)
    h = height
    return y1[:h] + ((y1[h : 2 * h] + y2[:h]) + (y1[2 * h :] + y2[h : 2 * h] + y3))


def apply_tiles(parts_ref, sums_ref, tiles_ref, rows_ref, cols_ref, count_ref, height, reach):
    row_tiles = sums_ref.shape[0]
    slots = tiles_ref.shape[0]
    base = rows_ref[0]
    count = count_ref[0]

    def diagonal(step, carry):
        for u in range(UNROLL):
            t = step * UNROLL + u
            sums_ref[t] = tile_product(parts_ref, tiles_ref, t, t + reach, height)
        return carry

    lax.fori_loop(0, row_tiles // UNROLL, diagonal, 0)

    def extra(step, carry):
        found = []
        for u in range(UNROLL):
            t = row_tiles + step * UNROLL + u
            y = tile_product(parts_ref, tiles_ref, t, cols_ref[t] - base + reach, height)
            found.append((rows_ref[t] - base, jnp.where(t < count, y, 0.0)))
        for row, y in found:
            sums_ref[row] += y
        return carry

    lax.fori_loop(0, (slots - row_tiles) // UNROLL, extra, 0)


def first_kernel(tile, rows_ref, cols_ref, count_ref, x_ref, left_ref, right_ref, tiles_ref,
                 image_ref, head_ref, tail_ref, parts_ref, sums_ref):
    channels = x_ref.shape[0]
    reach = left_ref.shape[1] // tile
    row_tiles = sums_ref.shape[0]
    load_span(parts_ref, 0, channels, left_ref, x_ref, right_ref, tile)
    apply_tiles(parts_ref, sums_ref, tiles_ref, rows_ref, cols_ref, count_ref, channels, reach)
    for i in range(row_tiles):
        cut = slice(i * tile, (i + 1) * tile)
        value = x_ref[:, cut] - sums_ref[i]
        image_ref[:, cut] = value
        if i < reach:
            head_ref[:, cut] = value
        if i >= row_tiles - reach:
            k = i - (row_tiles - reach)
            tail_ref[:, k * tile : (k + 1) * tile] = value


def iota2(shape, dim):
    return lax.broadcasted_iota(jnp.int32, shape, dim)


def dot_nt(a, b):
    return lax.dot_general(a, b, (((1,), (1,)), ((), ())), precision=HIGHEST,
                           preferred_element_type=F32)


def second_kernel(tile, rows_ref, cols_ref, count_ref, x_ref, p_ref, pleft_ref, pright_ref,
                  ax_ref, aleft_ref, aright_ref, tiles_ref, a2x_ref, message_ref,
                  parts_ref, sums_ref, basis_ref):
    k = x_ref.shape[0]
    reach = aleft_ref.shape[1] // tile
    row_tiles = sums_ref.shape[0]
    load_span(parts_ref, k, 2 * k, pleft_ref, p_ref, pright_ref, tile)
    load_span(parts_ref, 0, 2 * k, aleft_ref, ax_ref, aright_ref, tile)
    apply_tiles(parts_ref, sums_ref, tiles_ref, rows_ref, cols_ref, count_ref, 2 * k, reach)
    x = x_ref[...]
    ax = ax_ref[...]
    q = jnp.sum(x * ax, axis=1, keepdims=True) / (jnp.sum(x * x, axis=1, keepdims=True) + 1e-06)
    basis_ref[0:k, :] = x
    basis_ref[k : 2 * k, :] = ax - q * x
    basis_ref[2 * k : 3 * k, :] = p_ref[...]
    basis_ref[3 * k : 4 * k, :] = ax
    for i in range(row_tiles):
        cut = slice(i * tile, (i + 1) * tile)
        total = sums_ref[i]
        twice = ax_ref[:, cut] - total[:k]
        a2x_ref[:, cut] = twice
        basis_ref[4 * k : 5 * k, cut] = twice - q * ax_ref[:, cut]
        basis_ref[5 * k : 6 * k, cut] = p_ref[:, cut] - total[k:]
    grams = dot_nt(basis_ref[0 : 3 * k, :], basis_ref[...])
    message_ref[...] = jnp.zeros_like(message_ref)
    message_ref[:, 0 : 6 * k] = grams
    place = iota2((k, LANES), 1) == iota2((k, LANES), 0) + 6 * k
    message_ref[0:k, :] = jnp.where(place, q, message_ref[0:k, :])


def tree(values):
    while len(values) > 1:
        values = [values[i] + values[i + 1] for i in range(0, len(values), 2)]
    return values[0]


def merged(messages, k):
    lane = iota2((k, LANES), 1)
    row = iota2((k, LANES), 0)
    squares, crosses, quotients = [], [], []
    for m in messages:
        top = m[0:k]
        squares.append(jnp.sum(jnp.where(lane == row, top, 0.0), axis=1, keepdims=True))
        crosses.append(jnp.sum(jnp.where(lane == row + 3 * k, top, 0.0), axis=1, keepdims=True))
        quotients.append(jnp.sum(jnp.where(lane == row + 6 * k, top, 0.0), axis=1, keepdims=True))
    q = tree(crosses) / (tree(squares) + 1e-06)
    lane_all = iota2((3 * k, LANES), 1)
    shifted = []
    for m, own in zip(messages, quotients):
        move = own - q
        m = jnp.where(lane_all < 6 * k, m, 0.0)
        m = jnp.concatenate([m[0:k], m[k : 2 * k] + move * m[0:k], m[2 * k :]], axis=0)
        picks = (lane == row) | (lane == row + 3 * k)
        across = jnp.sum(jnp.where(picks, move, 0.0), axis=0, keepdims=True)
        shifted.append(m + pltpu.roll(m * across, k, 1))
    return tree(shifted), q


def merge_kernel(*refs):
    *ins, out_ref = refs
    k = out_ref.shape[0] // 3
    total, q = merged([r[...] for r in ins], k)
    out_ref[...] = total
    place = iota2((k, LANES), 1) == iota2((k, LANES), 0) + 6 * k
    out_ref[0:k, :] = jnp.where(place, q, total[0:k])


def eliminate(matrix):
    n = matrix.shape[0]
    blocks = [matrix[b : b + 8] for b in range(0, n, 8)]
    sub = iota2((8, LANES), 0)
    for j in range(n):
        b0, r0 = divmod(j, 8)
        line = blocks[b0][r0 : r0 + 1]
        pivot = line[:, j : j + 1]
        root = lax.rsqrt(pivot)
        root = root * (1.5 - 0.5 * pivot * root * root)
        line = line * root
        for b in range(b0, len(blocks)):
            update = blocks[b] - (blocks[b][:, j : j + 1] * root) * line
            if b == b0:
                update = jnp.where(sub > r0, update, jnp.where(sub == r0, line, blocks[b]))
            blocks[b] = update
    return jnp.concatenate(blocks, axis=0)


def inverse_factor(gram):
    n = gram.shape[0]
    wide = jnp.concatenate([gram, jnp.zeros((n, LANES - n), F32)], axis=1)
    wide = jnp.where(iota2((n, LANES), 1) == iota2((n, LANES), 0) + n, 1.0, wide)
    done = eliminate(wide)
    return pltpu.roll(done, LANES - n, 1)[:, 0:n]


def dot_nn(a, b):
    return jnp.dot(a, b, precision=HIGHEST, preferred_element_type=F32)


def last_kernel(count, scale, locked_ref, *refs):
    messages = refs[:count]
    x_ref, ax_ref, a2x_ref, w_ref, wi_ref, ritz_ref = refs[count:]
    k = x_ref.shape[0]
    locked = locked_ref[0]
    total, q = merged([r[...] for r in messages], k)
    total = total * scale
    plain = total[:, 0 : 3 * k]
    image = pltpu.roll(total, LANES - 3 * k, 1)[:, 0 : 3 * k]
    row = iota2((k, k), 0)
    col = iota2((k, k), 1)
    active = (row >= locked) & (col >= locked)
    frozen = (row == col) & (row < locked)
    residual_gram = pltpu.roll(total, LANES - k, 1)[k : 2 * k, 0:k]
    gram_w = jnp.where(active, residual_gram, 0.0) + jnp.where(frozen, 1.0, 0.0)
    inverse_w = jnp.where(active, inverse_factor(gram_w), 0.0)
    residual = ax_ref[...] - q * x_ref[...]
    w_ref[...] = dot_nn(inverse_w, residual)
    wi_ref[...] = dot_nn(inverse_w, a2x_ref[...] - q * ax_ref[...])
    zeros = jnp.zeros((k, LANES - k), F32)
    mid = pltpu.roll(jnp.concatenate([inverse_w, zeros], axis=1), k, 1)[:, 0 : 3 * k]
    row3 = iota2((3 * k, 3 * k), 0)
    col3 = iota2((3 * k, 3 * k), 1)
    same = row3 == col3
    middle = (row3 >= k) & (row3 < 2 * k)
    empty = jnp.zeros((k, 3 * k), F32)
    change = jnp.where(same & ~middle, 1.0, jnp.concatenate([empty, mid, empty], axis=0))
    gram_b = dot_nt(dot_nn(change, plain), change)
    pad = same & (row3 >= k) & (row3 < k + locked)
    gram_b = gram_b + jnp.where(pad, 1.0, 0.0)
    gram_a = dot_nt(dot_nn(change, image), change)
    symmetric = 0.5 * (gram_a + gram_a.T)
    inverse_b = inverse_factor(gram_b)
    ritz_ref[...] = dot_nt(dot_nn(inverse_b, symmetric), inverse_b)


def stages(members):
    found, stride = [], 1
    while stride < members:
        size = 4 if stride * 4 <= members else 2
        found.append((stride, size))
        stride *= size
    assert stride == members
    return found


def body(current_block, previous_block, adjacency_tiles, tile_rows, tile_cols, tile_count, locked):
    k, rows_here = current_block.shape
    slots, tile, _ = adjacency_tiles.shape
    members = lax.axis_size(AXES)
    vertex_total = rows_here * members
    row_tiles = rows_here // tile
    reach = row_tiles // 2
    width = reach * tile
    span = row_tiles + 2 * reach
    up = [(i, i + 1) for i in range(members - 1)]
    down = [(i + 1, i) for i in range(members - 1)]

    def halo(head, tail):
        return lax.ppermute(tail, AXES, up), lax.ppermute(head, AXES, down)

    def sds(*shape):
        return jax.ShapeDtypeStruct(shape, F32)

    left, right = halo(current_block[:, :width], current_block[:, rows_here - width :])
    pleft, pright = halo(previous_block[:, :width], previous_block[:, rows_here - width :])
    x_image, head, tail = pl.pallas_call(
        functools.partial(first_kernel, tile),
        out_shape=(sds(k, rows_here), sds(k, width), sds(k, width)),
        in_specs=[SMEM] * 3 + [VMEM] * 4,
        out_specs=(VMEM,) * 3,
        scratch_shapes=[
            pltpu.VMEM((span, 3 * k, tile), BF16),
            pltpu.VMEM((row_tiles, k, tile), F32),
        ],
        name="first_apply",
    )(tile_rows, tile_cols, tile_count, current_block, left, right, adjacency_tiles)
    aleft, aright = halo(head, tail)
    twice, message = pl.pallas_call(
        functools.partial(second_kernel, tile),
        out_shape=(sds(k, rows_here), sds(3 * k, LANES)),
        in_specs=[SMEM] * 3 + [VMEM] * 8,
        out_specs=(VMEM,) * 2,
        scratch_shapes=[
            pltpu.VMEM((span, 6 * k, tile), BF16),
            pltpu.VMEM((row_tiles, 2 * k, tile), F32),
            pltpu.VMEM((6 * k, rows_here), F32),
        ],
        name="second_apply",
    )(tile_rows, tile_cols, tile_count, current_block, previous_block, pleft, pright,
      x_image, aleft, aright, adjacency_tiles)
    plan = stages(members)
    for number, (stride, size) in enumerate(plan):
        messages = [message] + [
            lax.ppermute(message, AXES, [(i, i ^ (m * stride)) for i in range(members)])
            for m in range(1, size)
        ]
        if number < len(plan) - 1:
            message = pl.pallas_call(
                merge_kernel,
                out_shape=sds(3 * k, LANES),
                in_specs=[VMEM] * size,
                out_specs=VMEM,
                name="merge",
            )(*messages)
    return pl.pallas_call(
        functools.partial(last_kernel, len(messages), 1.0 / vertex_total),
        out_shape=(sds(k, rows_here), sds(k, rows_here), sds(3 * k, 3 * k)),
        in_specs=[SMEM] + [VMEM] * (len(messages) + 3),
        out_specs=(VMEM,) * 3,
        name="finish",
    )(locked, *messages, current_block, x_image, twice)


def solution(mesh):
    in_specs = (
        P(None, ("graphs", "rows", "cols", "sub")),
        P(None, ("graphs", "rows", "cols", "sub")),
        P(("graphs", "rows", "cols", "sub"), None, None),
        P(("graphs", "rows", "cols", "sub")),
        P(("graphs", "rows", "cols", "sub")),
        P(("graphs", "rows", "cols", "sub")),
        P("graphs"),
    )
    out_specs = (
        P(None, ("graphs", "rows", "cols", "sub")),
        P(None, ("graphs", "rows", "cols", "sub")),
        P("graphs", None),
    )
    return jax.shard_map(body, mesh=mesh, in_specs=in_specs, out_specs=out_specs, check_vma=False)
```

```python
import functools

import jax
import jax.numpy as jnp
from jax import lax
from jax.experimental import pallas as pl
from jax.experimental.pallas import tpu as pltpu
from jax.sharding import PartitionSpec as P

AXES = ("rows", "cols", "sub")
F32 = jnp.float32
BF16 = jnp.bfloat16
HIGHEST = lax.Precision.HIGHEST
LANES = 128
UNROLL = 8
GROUP = 4
VMEM_LIMIT = 24 * 1024 * 1024
VMEM = pl.BlockSpec(memory_space=pltpu.VMEM)
SMEM = pl.BlockSpec(memory_space=pltpu.SMEM)


def split3(x):
    a = x.astype(BF16)
    rest = x - a.astype(F32)
    b = rest.astype(BF16)
    c = (rest - b.astype(F32)).astype(BF16)
    return a, b, c


def store_parts(parts_ref, tile, at, height, values):
    channels = values.shape[0]
    for k, part in enumerate(split3(values)):
        parts_ref[tile, k * height + at : k * height + at + channels, :] = part


def load_span(parts_ref, at, height, left_ref, mid_ref, right_ref, tile):
    reach = left_ref.shape[1] // tile
    rows = mid_ref.shape[1] // tile
    for k in range(reach):
        cut = slice(k * tile, (k + 1) * tile)
        store_parts(parts_ref, k, at, height, left_ref[:, cut])
        store_parts(parts_ref, reach + rows + k, at, height, right_ref[:, cut])
    for k in range(rows):
        store_parts(parts_ref, reach + k, at, height, mid_ref[:, k * tile : (k + 1) * tile])


def tile_product(parts_ref, tiles_ref, t, col, height):
    lhs = parts_ref[col]
    t1, t2, t3 = tiles_ref[0, t], tiles_ref[1, t], tiles_ref[2, t]
    y1 = jnp.dot(lhs, t1, preferred_element_type=F32)
    y2 = jnp.dot(lhs[: 2 * height], t2, preferred_element_type=F32)
    y3 = jnp.dot(lhs[:height], t3, preferred_element_type=F32)
    h = height
    return y1[:h] + ((y1[h : 2 * h] + y2[:h]) + (y1[2 * h :] + y2[h : 2 * h] + y3))


def apply_tiles(parts_ref, sums_ref, tiles_ref, meta_ref, height, reach):
    row_tiles = sums_ref.shape[0]
    slots = tiles_ref.shape[1]
    base = meta_ref[0]
    count = meta_ref[2 * slots]

    def diagonal(step, carry):
        for u in range(UNROLL):
            t = step * UNROLL + u
            sums_ref[t] = tile_product(parts_ref, tiles_ref, t, t + reach, height)
        return carry

    lax.fori_loop(0, row_tiles // UNROLL, diagonal, 0)

    def extra(step, carry):
        found = []
        for u in range(UNROLL):
            t = row_tiles + step * UNROLL + u
            y = tile_product(parts_ref, tiles_ref, t, meta_ref[slots + t] - base + reach, height)
            found.append((meta_ref[t] - base, jnp.where(t < count, y, 0.0)))
        for row, y in found:
            sums_ref[row] += y
        return carry

    lax.fori_loop(0, (slots - row_tiles) // UNROLL, extra, 0)


def split_kernel(tiles_ref, out_ref):
    def step(t, carry):
        for u in range(2):
            for k, part in enumerate(split3(tiles_ref[2 * t + u])):
                out_ref[k, 2 * t + u] = part
        return carry

    lax.fori_loop(0, tiles_ref.shape[0] // 2, step, 0)


def first_kernel(tile, meta_ref, x_ref, left_ref, right_ref, tiles_ref,
                 image_ref, head_ref, tail_ref, parts_ref, sums_ref):
    channels = x_ref.shape[0]
    reach = left_ref.shape[1] // tile
    row_tiles = sums_ref.shape[0]
    load_span(parts_ref, 0, channels, left_ref.at[0:channels], x_ref, right_ref.at[0:channels], tile)
    apply_tiles(parts_ref, sums_ref, tiles_ref, meta_ref, channels, reach)
    for i in range(row_tiles):
        cut = slice(i * tile, (i + 1) * tile)
        value = x_ref[:, cut] - sums_ref[i]
        image_ref[:, cut] = value
        if i < reach:
            head_ref[:, cut] = value
        if i >= row_tiles - reach:
            k = i - (row_tiles - reach)
            tail_ref[:, k * tile : (k + 1) * tile] = value


def iota2(shape, dim):
    return lax.broadcasted_iota(jnp.int32, shape, dim)


def dot_nt(a, b):
    return lax.dot_general(a, b, (((1,), (1,)), ((), ())), precision=HIGHEST,
                           preferred_element_type=F32)


def second_kernel(tile, meta_ref, x_ref, p_ref, pleft_ref, pright_ref,
                  ax_ref, aleft_ref, aright_ref, tiles_ref, a2x_ref, message_ref,
                  parts_ref, sums_ref, basis_ref):
    k = x_ref.shape[0]
    reach = aleft_ref.shape[1] // tile
    row_tiles = sums_ref.shape[0]
    load_span(parts_ref, k, 2 * k, pleft_ref.at[k : 2 * k], p_ref, pright_ref.at[k : 2 * k], tile)
    load_span(parts_ref, 0, 2 * k, aleft_ref, ax_ref, aright_ref, tile)
    apply_tiles(parts_ref, sums_ref, tiles_ref, meta_ref, 2 * k, reach)
    x = x_ref[...]
    ax = ax_ref[...]
    q = jnp.sum(x * ax, axis=1, keepdims=True) / (jnp.sum(x * x, axis=1, keepdims=True) + 1e-06)
    basis_ref[0:k, :] = x
    basis_ref[k : 2 * k, :] = ax - q * x
    basis_ref[2 * k : 3 * k, :] = p_ref[...]
    basis_ref[3 * k : 4 * k, :] = ax
    for i in range(row_tiles):
        cut = slice(i * tile, (i + 1) * tile)
        total = sums_ref[i]
        twice = ax_ref[:, cut] - total[:k]
        a2x_ref[:, cut] = twice
        basis_ref[4 * k : 5 * k, cut] = twice - q * ax_ref[:, cut]
        basis_ref[5 * k : 6 * k, cut] = p_ref[:, cut] - total[k:]
    grams = dot_nt(basis_ref[0 : 3 * k, :], basis_ref[...])
    message_ref[...] = jnp.zeros_like(message_ref)
    message_ref[:, 0 : 6 * k] = grams
    place = iota2((k, LANES), 1) == iota2((k, LANES), 0) + 6 * k
    message_ref[0:k, :] = jnp.where(place, q, message_ref[0:k, :])


def tree(values):
    while len(values) > 1:
        values = [values[i] + values[i + 1] for i in range(0, len(values), 2)]
    return values[0]


def merged(messages, k):
    lane = iota2((k, LANES), 1)
    row = iota2((k, LANES), 0)
    squares, crosses, quotients = [], [], []
    for m in messages:
        top = m[0:k]
        squares.append(jnp.sum(jnp.where(lane == row, top, 0.0), axis=1, keepdims=True))
        crosses.append(jnp.sum(jnp.where(lane == row + 3 * k, top, 0.0), axis=1, keepdims=True))
        quotients.append(jnp.sum(jnp.where(lane == row + 6 * k, top, 0.0), axis=1, keepdims=True))
    q = tree(crosses) / (tree(squares) + 1e-06)
    lane_all = iota2((3 * k, LANES), 1)
    shifted = []
    for m, own in zip(messages, quotients):
        move = own - q
        m = jnp.where(lane_all < 6 * k, m, 0.0)
        m = jnp.concatenate([m[0:k], m[k : 2 * k] + move * m[0:k], m[2 * k :]], axis=0)
        picks = (lane == row) | (lane == row + 3 * k)
        across = jnp.sum(jnp.where(picks, move, 0.0), axis=0, keepdims=True)
        shifted.append(m + pltpu.roll(m * across, k, 1))
    return tree(shifted), q


def merge_kernel(*refs):
    *ins, out_ref = refs
    k = out_ref.shape[0] // 3
    total, q = merged([r[...] for r in ins], k)
    out_ref[...] = total
    place = iota2((k, LANES), 1) == iota2((k, LANES), 0) + 6 * k
    out_ref[0:k, :] = jnp.where(place, q, total[0:k])


def eliminate(matrix):
    n = matrix.shape[0]
    full = (8, LANES)
    blocks = [matrix[b : b + 8] for b in range(0, n, 8)]
    sub = iota2(full, 0)
    for g in range(0, n, GROUP):
        b0, r0 = divmod(g, 8)
        rows = [jnp.broadcast_to(blocks[b0][r0 + i : r0 + i + 1], full) for i in range(GROUP)]
        s = [[jnp.broadcast_to(rows[i][:, g + l : g + l + 1], full) if l >= i else None
              for l in range(GROUP)] for i in range(GROUP)]
        cols = {b: [jnp.broadcast_to(blocks[b][:, g + i : g + i + 1], full) for i in range(GROUP)]
                for b in range(b0, len(blocks))}
        for a in range(GROUP):
            inverse = 1.0 / s[a][a]
            for l in range(a + 1, GROUP):
                f = s[a][l] * inverse
                for c in range(l, GROUP):
                    s[l][c] = s[l][c] - f * s[a][c]
                rows[l] = rows[l] - f * rows[a]
                for b in cols:
                    cols[b][l] = cols[b][l] - f * cols[b][a]
            for b in cols:
                cols[b][a] = cols[b][a] * inverse
        for b in cols:
            update = blocks[b]
            for a in range(GROUP):
                update = update - cols[b][a] * rows[a]
            if b == b0:
                update = jnp.where(sub >= r0 + GROUP, update, blocks[b])
                for a in range(GROUP):
                    root = lax.rsqrt(s[a][a])
                    root = root * (1.5 - 0.5 * s[a][a] * root * root)
                    update = jnp.where(sub == r0 + a, rows[a] * root, update)
            blocks[b] = update
    return jnp.concatenate(blocks, axis=0)


def inverse_factor(gram):
    n = gram.shape[0]
    wide = jnp.concatenate([gram, jnp.zeros((n, LANES - n), F32)], axis=1)
    wide = jnp.where(iota2((n, LANES), 1) == iota2((n, LANES), 0) + n, 1.0, wide)
    done = eliminate(wide)
    return pltpu.roll(done, LANES - n, 1)[:, 0:n]


def dot_nn(a, b):
    return jnp.dot(a, b, precision=HIGHEST, preferred_element_type=F32)


def last_kernel(count, scale, locked_ref, *refs):
    messages = refs[:count]
    x_ref, ax_ref, a2x_ref, w_ref, wi_ref, ritz_ref = refs[count:]
    k = x_ref.shape[0]
    locked = locked_ref[0]
    total, q = merged([r[...] for r in messages], k)
    total = total * scale
    plain = total[:, 0 : 3 * k]
    image = pltpu.roll(total, LANES - 3 * k, 1)[:, 0 : 3 * k]
    row = iota2((k, k), 0)
    col = iota2((k, k), 1)
    active = (row >= locked) & (col >= locked)
    frozen = (row == col) & (row < locked)
    residual_gram = pltpu.roll(total, LANES - k, 1)[k : 2 * k, 0:k]
    gram_w = jnp.where(active, residual_gram, 0.0) + jnp.where(frozen, 1.0, 0.0)
    inverse_w = jnp.where(active, inverse_factor(gram_w), 0.0)
    residual = ax_ref[...] - q * x_ref[...]
    w_ref[...] = dot_nn(inverse_w, residual)
    wi_ref[...] = dot_nn(inverse_w, a2x_ref[...] - q * ax_ref[...])
    zeros = jnp.zeros((k, LANES - k), F32)
    mid = pltpu.roll(jnp.concatenate([inverse_w, zeros], axis=1), k, 1)[:, 0 : 3 * k]
    row3 = iota2((3 * k, 3 * k), 0)
    col3 = iota2((3 * k, 3 * k), 1)
    same = row3 == col3
    middle = (row3 >= k) & (row3 < 2 * k)
    empty = jnp.zeros((k, 3 * k), F32)
    change = jnp.where(same & ~middle, 1.0, jnp.concatenate([empty, mid, empty], axis=0))
    gram_b = dot_nt(dot_nn(change, plain), change)
    pad = same & (row3 >= k) & (row3 < k + locked)
    gram_b = gram_b + jnp.where(pad, 1.0, 0.0)
    gram_a = dot_nt(dot_nn(change, image), change)
    symmetric = 0.5 * (gram_a + gram_a.T)
    inverse_b = inverse_factor(gram_b)
    ritz_ref[...] = dot_nt(dot_nn(inverse_b, symmetric), inverse_b)


def stages(members):
    found, stride = [], 1
    while stride < members:
        size = 2
        found.append((stride, size))
        stride *= size
    assert stride == members
    return found


def body(current_block, previous_block, adjacency_tiles, tile_rows, tile_cols, tile_count, locked):
    k, rows_here = current_block.shape
    slots, tile, _ = adjacency_tiles.shape
    members = lax.axis_size(AXES)
    vertex_total = rows_here * members
    row_tiles = rows_here // tile
    reach = row_tiles // 2
    width = reach * tile
    span = row_tiles + 2 * reach
    up = [(i, i + 1) for i in range(members - 1)]
    down = [(i + 1, i) for i in range(members - 1)]

    meta = jnp.concatenate([tile_rows, tile_cols, tile_count])

    def halo(head, tail):
        return lax.ppermute(tail, AXES, up), lax.ppermute(head, AXES, down)

    def sds(*shape):
        return jax.ShapeDtypeStruct(shape, F32)

    cut = rows_here - width
    left, right = halo(
        jnp.concatenate([current_block[:, :width], previous_block[:, :width]], axis=0),
        jnp.concatenate([current_block[:, cut:], previous_block[:, cut:]], axis=0),
    )
    parts = pl.pallas_call(
        split_kernel,
        out_shape=jax.ShapeDtypeStruct((3, slots, tile, tile), BF16),
        in_specs=[VMEM],
        out_specs=VMEM,
        compiler_params=pltpu.CompilerParams(vmem_limit_bytes=VMEM_LIMIT),
        cost_estimate=pl.CostEstimate(flops=10**8, bytes_accessed=10**7, transcendentals=0),
        name="split_tiles",
    )(adjacency_tiles)
    x_image, head, tail = pl.pallas_call(
        functools.partial(first_kernel, tile),
        out_shape=(sds(k, rows_here), sds(k, width), sds(k, width)),
        in_specs=[SMEM] + [VMEM] * 4,
        out_specs=(VMEM,) * 3,
        scratch_shapes=[
            pltpu.VMEM((span, 3 * k, tile), BF16),
            pltpu.VMEM((row_tiles, k, tile), F32),
        ],
        compiler_params=pltpu.CompilerParams(vmem_limit_bytes=VMEM_LIMIT),
        name="first_apply",
    )(meta, current_block, left, right, parts)
    aleft, aright = halo(head, tail)
    twice, message = pl.pallas_call(
        functools.partial(second_kernel, tile),
        out_shape=(sds(k, rows_here), sds(3 * k, LANES)),
        in_specs=[SMEM] + [VMEM] * 8,
        out_specs=(VMEM,) * 2,
        scratch_shapes=[
            pltpu.VMEM((span, 6 * k, tile), BF16),
            pltpu.VMEM((row_tiles, 2 * k, tile), F32),
            pltpu.VMEM((6 * k, rows_here), F32),
        ],
        compiler_params=pltpu.CompilerParams(vmem_limit_bytes=VMEM_LIMIT),
        name="second_apply",
    )(meta, current_block, previous_block, left, right,
      x_image, aleft, aright, parts)
    plan = stages(members)
    for number, (stride, size) in enumerate(plan):
        messages = [message] + [
            lax.ppermute(message, AXES, [(i, i ^ (m * stride)) for i in range(members)])
            for m in range(1, size)
        ]
        if number < len(plan) - 1:
            message = pl.pallas_call(
                merge_kernel,
                out_shape=sds(3 * k, LANES),
                in_specs=[VMEM] * size,
                out_specs=VMEM,
                compiler_params=pltpu.CompilerParams(vmem_limit_bytes=VMEM_LIMIT),
        name="merge",
            )(*messages)
    return pl.pallas_call(
        functools.partial(last_kernel, len(messages), 1.0 / vertex_total),
        out_shape=(sds(k, rows_here), sds(k, rows_here), sds(3 * k, 3 * k)),
        in_specs=[SMEM] + [VMEM] * (len(messages) + 3),
        out_specs=(VMEM,) * 3,
        compiler_params=pltpu.CompilerParams(vmem_limit_bytes=VMEM_LIMIT),
        name="finish",
    )(locked, *messages, current_block, x_image, twice)


def solution(mesh):
    in_specs = (
        P(None, ("graphs", "rows", "cols", "sub")),
        P(None, ("graphs", "rows", "cols", "sub")),
        P(("graphs", "rows", "cols", "sub"), None, None),
        P(("graphs", "rows", "cols", "sub")),
        P(("graphs", "rows", "cols", "sub")),
        P(("graphs", "rows", "cols", "sub")),
        P("graphs"),
    )
    out_specs = (
        P(None, ("graphs", "rows", "cols", "sub")),
        P(None, ("graphs", "rows", "cols", "sub")),
        P("graphs", None),
    )
    return jax.shard_map(body, mesh=mesh, in_specs=in_specs, out_specs=out_specs, check_vma=False)
```

```python
import functools

import jax
import jax.numpy as jnp
from jax import lax
from jax.experimental import pallas as pl
from jax.experimental.pallas import tpu as pltpu
from jax.sharding import PartitionSpec as P

AXES = ("rows", "cols", "sub")
F32 = jnp.float32
BF16 = jnp.bfloat16
HIGHEST = lax.Precision.HIGHEST
LANES = 128
UNROLL = 8
GROUP = 8
VMEM_LIMIT = 24 * 1024 * 1024
VMEM = pl.BlockSpec(memory_space=pltpu.VMEM)
SMEM = pl.BlockSpec(memory_space=pltpu.SMEM)


def split3(x):
    a = x.astype(BF16)
    rest = x - a.astype(F32)
    b = rest.astype(BF16)
    c = (rest - b.astype(F32)).astype(BF16)
    return a, b, c


def store_parts(parts_ref, tile, at, height, values):
    channels = values.shape[0]
    for k, part in enumerate(split3(values)):
        parts_ref[tile, k * height + at : k * height + at + channels, :] = part


def load_edges(parts_ref, at, height, first_ref, second_ref, rows, tile, odd):
    reach = first_ref.shape[1] // tile
    first = jnp.where(odd, 0, reach + rows)
    second = reach + rows - first
    for k in range(reach):
        cut = slice(k * tile, (k + 1) * tile)
        store_parts(parts_ref, first + k, at, height, first_ref[:, cut])
        store_parts(parts_ref, second + k, at, height, second_ref[:, cut])


def load_middle(parts_ref, offset, at, height, mid_ref, tile):
    for k in range(mid_ref.shape[1] // tile):
        store_parts(parts_ref, offset + k, at, height, mid_ref[:, k * tile : (k + 1) * tile])


def tile_product(parts_ref, tiles_ref, t, col, height):
    lhs = parts_ref[col]
    t1, t2, t3 = tiles_ref[0, t], tiles_ref[1, t], tiles_ref[2, t]
    y1 = jnp.dot(lhs, t1, preferred_element_type=F32)
    y2 = jnp.dot(lhs[: 2 * height], t2, preferred_element_type=F32)
    y3 = jnp.dot(lhs[:height], t3, preferred_element_type=F32)
    h = height
    return y1[:h] + ((y1[h : 2 * h] + y2[:h]) + (y1[2 * h :] + y2[h : 2 * h] + y3))


def diagonal_tiles(parts_ref, sums_ref, tiles_ref, height, start, stop):
    def step(index, carry):
        for u in range(UNROLL):
            t = index * UNROLL + u
            sums_ref[t] = tile_product(parts_ref, tiles_ref, t, t, height)
        return carry

    lax.fori_loop(start // UNROLL, stop // UNROLL, step, 0)


def extra_tiles(parts_ref, sums_ref, tiles_ref, meta_ref, height, reach):
    row_tiles = sums_ref.shape[0]
    slots = tiles_ref.shape[1]
    base = meta_ref[0]
    count = meta_ref[2 * slots]

    def step(index, carry):
        found = []
        for u in range(UNROLL):
            t = row_tiles + index * UNROLL + u
            y = tile_product(parts_ref, tiles_ref, t, meta_ref[slots + t] - base + reach, height)
            found.append((meta_ref[t] - base, jnp.where(t < count, y, 0.0)))
        for row, y in found:
            sums_ref[row] += y
        return carry

    lax.fori_loop(0, (slots - row_tiles) // UNROLL, step, 0)


def split_kernel(tiles_hbm, x_ref, out_ref, sums_ref, tiles_ref, parts_ref, sems):
    row_tiles, k_rows, tile = sums_ref.shape
    slots = tiles_ref.shape[0]
    chunks = sems.shape[0]
    size = slots // chunks

    def copy(c):
        part = pl.ds(c * size, size)
        return pltpu.make_async_copy(tiles_hbm.at[part], tiles_ref.at[part], sems.at[c])

    for c in range(chunks):
        copy(c).start()
    load_middle(parts_ref, 0, 0, k_rows, x_ref, tile)
    for c in range(chunks):
        copy(c).wait()

        def step(t, carry):
            for k, part in enumerate(split3(tiles_ref[t])):
                out_ref[k, t] = part
            return carry

        lax.fori_loop(c * size, (c + 1) * size, step, 0, unroll=2)
        if (c + 1) * size <= row_tiles:
            diagonal_tiles(parts_ref, sums_ref, out_ref, k_rows, c * size, (c + 1) * size)


def first_kernel(tile, meta_ref, x_ref, left_ref, right_ref, tiles_ref, start_ref,
                 image_ref, first_ref, second_ref, parts_ref, sums_ref):
    channels = x_ref.shape[0]
    reach = left_ref.shape[1] // tile
    row_tiles = sums_ref.shape[0]
    odd = meta_ref[2 * tiles_ref.shape[1] + 1] == 1
    load_middle(parts_ref, reach, 0, channels, x_ref, tile)
    load_edges(parts_ref, 0, channels, left_ref.at[0:channels], right_ref.at[0:channels],
               row_tiles, tile, odd)
    sums_ref[...] = start_ref[...]
    extra_tiles(parts_ref, sums_ref, tiles_ref, meta_ref, channels, reach)
    for i in range(row_tiles):
        cut = slice(i * tile, (i + 1) * tile)
        image_ref[:, cut] = x_ref[:, cut] - sums_ref[i]
    far = (row_tiles - reach) * tile
    head = image_ref[:, : reach * tile]
    tail = image_ref[:, far:]
    first_ref[...] = jnp.where(odd, head, tail)
    second_ref[...] = jnp.where(odd, tail, head)


def iota2(shape, dim):
    return lax.broadcasted_iota(jnp.int32, shape, dim)


def dot_nt(a, b):
    return lax.dot_general(a, b, (((1,), (1,)), ((), ())), precision=HIGHEST,
                           preferred_element_type=F32)


def middle_kernel(tile, x_ref, p_ref, ax_ref, tiles_ref,
                  sums_ref, basis_ref, quotient_ref, message_ref, parts_ref):
    k = x_ref.shape[0]
    load_middle(parts_ref, 0, 0, 2 * k, ax_ref, tile)
    load_middle(parts_ref, 0, k, 2 * k, p_ref, tile)
    diagonal_tiles(parts_ref, sums_ref, tiles_ref, 2 * k, 0, sums_ref.shape[0])
    x = x_ref[...]
    ax = ax_ref[...]
    q = jnp.sum(x * ax, axis=1, keepdims=True) / (jnp.sum(x * x, axis=1, keepdims=True) + 1e-06)
    basis_ref[0:k, :] = x
    basis_ref[k : 2 * k, :] = ax - q * x
    basis_ref[2 * k : 3 * k, :] = p_ref[...]
    basis_ref[3 * k : 4 * k, :] = ax
    quotient_ref[...] = jnp.broadcast_to(q, quotient_ref.shape)
    message_ref[...] = jnp.zeros_like(message_ref)
    message_ref[:, 0 : 4 * k] = dot_nt(basis_ref[0 : 3 * k, :], basis_ref[...])
    place = iota2((k, LANES), 1) == iota2((k, LANES), 0) + 6 * k
    message_ref[0:k, :] = jnp.where(place, q, message_ref[0:k, :])


def second_kernel(tile, meta_ref, p_ref, pleft_ref, pright_ref, ax_ref, aleft_ref, aright_ref,
                  tiles_ref, start_ref, basis_ref, quotient_ref, begun_ref,
                  a2x_ref, message_ref, parts_ref, sums_ref, images_ref):
    k = p_ref.shape[0]
    reach = aleft_ref.shape[1] // tile
    row_tiles = sums_ref.shape[0]
    odd = meta_ref[2 * tiles_ref.shape[1] + 1] == 1
    load_middle(parts_ref, reach, 0, 2 * k, ax_ref, tile)
    load_middle(parts_ref, reach, k, 2 * k, p_ref, tile)
    load_edges(parts_ref, k, 2 * k, pleft_ref.at[k : 2 * k], pright_ref.at[k : 2 * k],
               row_tiles, tile, odd)
    load_edges(parts_ref, 0, 2 * k, aleft_ref, aright_ref, row_tiles, tile, odd)
    sums_ref[...] = start_ref[...]
    extra_tiles(parts_ref, sums_ref, tiles_ref, meta_ref, 2 * k, reach)
    q = quotient_ref[:, 0:1]
    for i in range(row_tiles):
        cut = slice(i * tile, (i + 1) * tile)
        total = sums_ref[i]
        twice = ax_ref[:, cut] - total[:k]
        a2x_ref[:, cut] = twice
        images_ref[0:k, cut] = twice - q * ax_ref[:, cut]
        images_ref[k : 2 * k, cut] = p_ref[:, cut] - total[k:]
    message_ref[...] = begun_ref[...]
    message_ref[:, 4 * k : 6 * k] = dot_nt(basis_ref[0 : 3 * k, :], images_ref[...])


def tree(values):
    while len(values) > 1:
        values = [values[i] + values[i + 1] for i in range(0, len(values), 2)]
    return values[0]


def merged(messages, k):
    lane = iota2((k, LANES), 1)
    row = iota2((k, LANES), 0)
    squares, crosses, quotients = [], [], []
    for m in messages:
        top = m[0:k]
        squares.append(jnp.sum(jnp.where(lane == row, top, 0.0), axis=1, keepdims=True))
        crosses.append(jnp.sum(jnp.where(lane == row + 3 * k, top, 0.0), axis=1, keepdims=True))
        quotients.append(jnp.sum(jnp.where(lane == row + 6 * k, top, 0.0), axis=1, keepdims=True))
    q = tree(crosses) / (tree(squares) + 1e-06)
    lane_all = iota2((3 * k, LANES), 1)
    shifted = []
    for m, own in zip(messages, quotients):
        move = own - q
        m = jnp.where(lane_all < 6 * k, m, 0.0)
        m = jnp.concatenate([m[0:k], m[k : 2 * k] + move * m[0:k], m[2 * k :]], axis=0)
        picks = (lane == row) | (lane == row + 3 * k)
        across = jnp.sum(jnp.where(picks, move, 0.0), axis=0, keepdims=True)
        shifted.append(m + pltpu.roll(m * across, k, 1))
    return tree(shifted), q


def merge_kernel(*refs):
    *ins, out_ref = refs
    k = out_ref.shape[0] // 3
    total, q = merged([r[...] for r in ins], k)
    out_ref[...] = total
    place = iota2((k, LANES), 1) == iota2((k, LANES), 0) + 6 * k
    out_ref[0:k, :] = jnp.where(place, q, total[0:k])


def eliminate(matrix):
    n = matrix.shape[0]
    full = (8, LANES)
    blocks = [matrix[b : b + 8] for b in range(0, n, 8)]
    sub = iota2(full, 0)
    for g in range(0, n, GROUP):
        b0, r0 = divmod(g, 8)
        rows = [jnp.broadcast_to(blocks[b0][r0 + i : r0 + i + 1], full) for i in range(GROUP)]
        s = [[jnp.broadcast_to(rows[i][:, g + l : g + l + 1], full) if l >= i else None
              for l in range(GROUP)] for i in range(GROUP)]
        cols = {b: [jnp.broadcast_to(blocks[b][:, g + i : g + i + 1], full) for i in range(GROUP)]
                for b in range(b0, len(blocks))}
        for a in range(GROUP):
            inverse = 1.0 / s[a][a]
            for l in range(a + 1, GROUP):
                f = s[a][l] * inverse
                for c in range(l, GROUP):
                    s[l][c] = s[l][c] - f * s[a][c]
                rows[l] = rows[l] - f * rows[a]
                for b in cols:
                    cols[b][l] = cols[b][l] - f * cols[b][a]
            for b in cols:
                cols[b][a] = cols[b][a] * inverse
        for b in cols:
            update = blocks[b]
            for a in range(GROUP):
                update = update - cols[b][a] * rows[a]
            if b == b0:
                update = jnp.where(sub >= r0 + GROUP, update, blocks[b])
                for a in range(GROUP):
                    root = lax.rsqrt(s[a][a])
                    root = root * (1.5 - 0.5 * s[a][a] * root * root)
                    update = jnp.where(sub == r0 + a, rows[a] * root, update)
            blocks[b] = update
    return jnp.concatenate(blocks, axis=0)


def inverse_factor(gram):
    n = gram.shape[0]
    wide = jnp.concatenate([gram, jnp.zeros((n, LANES - n), F32)], axis=1)
    wide = jnp.where(iota2((n, LANES), 1) == iota2((n, LANES), 0) + n, 1.0, wide)
    done = eliminate(wide)
    return pltpu.roll(done, LANES - n, 1)[:, 0:n]


def dot_nn(a, b):
    return jnp.dot(a, b, precision=HIGHEST, preferred_element_type=F32)


def last_kernel(count, scale, locked_ref, *refs):
    messages = refs[:count]
    x_ref, ax_ref, a2x_ref, w_ref, wi_ref, ritz_ref = refs[count:]
    k = x_ref.shape[0]
    locked = locked_ref[0]
    total, q = merged([r[...] for r in messages], k)
    total = total * scale
    plain = total[:, 0 : 3 * k]
    image = pltpu.roll(total, LANES - 3 * k, 1)[:, 0 : 3 * k]
    row = iota2((k, k), 0)
    col = iota2((k, k), 1)
    active = (row >= locked) & (col >= locked)
    frozen = (row == col) & (row < locked)
    residual_gram = pltpu.roll(total, LANES - k, 1)[k : 2 * k, 0:k]
    gram_w = jnp.where(active, residual_gram, 0.0) + jnp.where(frozen, 1.0, 0.0)
    inverse_w = jnp.where(active, inverse_factor(gram_w), 0.0)
    residual = ax_ref[...] - q * x_ref[...]
    w_ref[...] = dot_nn(inverse_w, residual)
    wi_ref[...] = dot_nn(inverse_w, a2x_ref[...] - q * ax_ref[...])
    zeros = jnp.zeros((k, LANES - k), F32)
    mid = pltpu.roll(jnp.concatenate([inverse_w, zeros], axis=1), k, 1)[:, 0 : 3 * k]
    row3 = iota2((3 * k, 3 * k), 0)
    col3 = iota2((3 * k, 3 * k), 1)
    same = row3 == col3
    middle = (row3 >= k) & (row3 < 2 * k)
    empty = jnp.zeros((k, 3 * k), F32)
    change = jnp.where(same & ~middle, 1.0, jnp.concatenate([empty, mid, empty], axis=0))
    gram_b = dot_nt(dot_nn(change, plain), change)
    pad = same & (row3 >= k) & (row3 < k + locked)
    gram_b = gram_b + jnp.where(pad, 1.0, 0.0)
    gram_a = dot_nt(dot_nn(change, image), change)
    symmetric = 0.5 * (gram_a + gram_a.T)
    inverse_b = inverse_factor(gram_b)
    ritz_ref[...] = dot_nt(dot_nn(inverse_b, symmetric), inverse_b)


def stages(members):
    found, stride = [], 1
    while stride < members:
        size = 2
        found.append((stride, size))
        stride *= size
    assert stride == members
    return found


def body(current_block, previous_block, adjacency_tiles, tile_rows, tile_cols, tile_count, locked):
    k, rows_here = current_block.shape
    slots, tile, _ = adjacency_tiles.shape
    members = lax.axis_size(AXES)
    vertex_total = rows_here * members
    row_tiles = rows_here // tile
    reach = row_tiles // 2
    width = reach * tile
    span = row_tiles + 2 * reach
    inner = [(i, i ^ 1) for i in range(members)]
    outer = [(i, i + 1 if i % 2 else i - 1) for i in range(1, members - 1)]
    odd = lax.axis_index(AXES) % 2
    meta = jnp.concatenate([tile_rows, tile_cols, tile_count, odd[None].astype(jnp.int32)])

    def halo(first, second):
        return lax.ppermute(first, AXES, inner), lax.ppermute(second, AXES, outer)

    def sds(*shape):
        return jax.ShapeDtypeStruct(shape, F32)

    def edge(start):
        return jnp.concatenate(
            [
                lax.dynamic_slice_in_dim(block, start * (rows_here - width), width, 1)
                for block in (current_block, previous_block)
            ],
            axis=0,
        )

    left, right = halo(edge(1 - odd), edge(odd))
    params = pltpu.CompilerParams(vmem_limit_bytes=VMEM_LIMIT)
    cost = pl.CostEstimate(flops=10**8, bytes_accessed=10**7, transcendentals=0)
    parts, x_sums = pl.pallas_call(
        split_kernel,
        out_shape=(jax.ShapeDtypeStruct((3, slots, tile, tile), BF16), sds(row_tiles, k, tile)),
        in_specs=[pl.BlockSpec(memory_space=pltpu.HBM), VMEM],
        out_specs=(VMEM,) * 2,
        scratch_shapes=[
            pltpu.VMEM((slots, tile, tile), F32),
            pltpu.VMEM((row_tiles, 3 * k, tile), BF16),
            pltpu.SemaphoreType.DMA((slots // UNROLL,)),
        ],
        compiler_params=params,
        cost_estimate=cost,
        name="split_tiles",
    )(adjacency_tiles, current_block)
    x_image, head, tail = pl.pallas_call(
        functools.partial(first_kernel, tile),
        out_shape=(sds(k, rows_here), sds(k, width), sds(k, width)),
        in_specs=[SMEM] + [VMEM] * 5,
        out_specs=(VMEM,) * 3,
        scratch_shapes=[
            pltpu.VMEM((span, 3 * k, tile), BF16),
            pltpu.VMEM((row_tiles, k, tile), F32),
        ],
        compiler_params=params,
        name="first_apply",
    )(meta, current_block, left, right, parts, x_sums)
    aleft, aright = halo(head, tail)
    sums, basis, quotient, begun = pl.pallas_call(
        functools.partial(middle_kernel, tile),
        out_shape=(sds(row_tiles, 2 * k, tile), sds(4 * k, rows_here), sds(k, LANES),
                   sds(3 * k, LANES)),
        in_specs=[VMEM] * 4,
        out_specs=(VMEM,) * 4,
        scratch_shapes=[pltpu.VMEM((row_tiles, 6 * k, tile), BF16)],
        compiler_params=params,
        cost_estimate=cost,
        name="middle",
    )(current_block, previous_block, x_image, parts)
    twice, message = pl.pallas_call(
        functools.partial(second_kernel, tile),
        out_shape=(sds(k, rows_here), sds(3 * k, LANES)),
        in_specs=[SMEM] + [VMEM] * 11,
        out_specs=(VMEM,) * 2,
        scratch_shapes=[
            pltpu.VMEM((span, 6 * k, tile), BF16),
            pltpu.VMEM((row_tiles, 2 * k, tile), F32),
            pltpu.VMEM((2 * k, rows_here), F32),
        ],
        compiler_params=params,
        name="second_apply",
    )(meta, previous_block, left, right, x_image, aleft, aright, parts, sums, basis, quotient,
      begun)
    plan = stages(members)
    for number, (stride, size) in enumerate(plan):
        messages = [message] + [
            lax.ppermute(message, AXES, [(i, i ^ (m * stride)) for i in range(members)])
            for m in range(1, size)
        ]
        if number < len(plan) - 1:
            message = pl.pallas_call(
                merge_kernel,
                out_shape=sds(3 * k, LANES),
                in_specs=[VMEM] * size,
                out_specs=VMEM,
                compiler_params=pltpu.CompilerParams(vmem_limit_bytes=VMEM_LIMIT),
        name="merge",
            )(*messages)
    return pl.pallas_call(
        functools.partial(last_kernel, len(messages), 1.0 / vertex_total),
        out_shape=(sds(k, rows_here), sds(k, rows_here), sds(3 * k, 3 * k)),
        in_specs=[SMEM] + [VMEM] * (len(messages) + 3),
        out_specs=(VMEM,) * 3,
        compiler_params=pltpu.CompilerParams(vmem_limit_bytes=VMEM_LIMIT),
        name="finish",
    )(locked, *messages, current_block, x_image, twice)


def solution(mesh):
    in_specs = (
        P(None, ("graphs", "rows", "cols", "sub")),
        P(None, ("graphs", "rows", "cols", "sub")),
        P(("graphs", "rows", "cols", "sub"), None, None),
        P(("graphs", "rows", "cols", "sub")),
        P(("graphs", "rows", "cols", "sub")),
        P(("graphs", "rows", "cols", "sub")),
        P("graphs"),
    )
    out_specs = (
        P(None, ("graphs", "rows", "cols", "sub")),
        P(None, ("graphs", "rows", "cols", "sub")),
        P("graphs", None),
    )
    return jax.shard_map(body, mesh=mesh, in_specs=in_specs, out_specs=out_specs, check_vma=False)
```

```python
import functools

import jax
import jax.numpy as jnp
from jax import lax
from jax.experimental import pallas as pl
from jax.experimental.pallas import tpu as pltpu
from jax.sharding import PartitionSpec as P

AXES = ("rows", "cols", "sub")
F32 = jnp.float32
BF16 = jnp.bfloat16
HIGHEST = lax.Precision.HIGHEST
LANES = 128
UNROLL = 8
GROUP = 8
VMEM_LIMIT = 24 * 1024 * 1024
VMEM = pl.BlockSpec(memory_space=pltpu.VMEM)
SMEM = pl.BlockSpec(memory_space=pltpu.SMEM)


def split3(x):
    a = x.astype(BF16)
    rest = x - a.astype(F32)
    b = rest.astype(BF16)
    c = (rest - b.astype(F32)).astype(BF16)
    return a, b, c


def store_parts(parts_ref, tile, at, height, values):
    channels = values.shape[0]
    for k, part in enumerate(split3(values)):
        parts_ref[tile, k * height + at : k * height + at + channels, :] = part


def load_edges(parts_ref, at, height, first_ref, second_ref, rows, tile, odd):
    reach = first_ref.shape[1] // tile
    first = jnp.where(odd, 0, reach + rows)
    second = reach + rows - first
    for k in range(reach):
        cut = slice(k * tile, (k + 1) * tile)
        store_parts(parts_ref, first + k, at, height, first_ref[:, cut])
        store_parts(parts_ref, second + k, at, height, second_ref[:, cut])


def load_middle(parts_ref, offset, at, height, mid_ref, tile):
    for k in range(mid_ref.shape[1] // tile):
        store_parts(parts_ref, offset + k, at, height, mid_ref[:, k * tile : (k + 1) * tile])


def tile_product(parts_ref, tiles_ref, t, col, height):
    lhs = parts_ref[col]
    t1, t2, t3 = tiles_ref[0, t], tiles_ref[1, t], tiles_ref[2, t]
    y1 = jnp.dot(lhs, t1, preferred_element_type=F32)
    y2 = jnp.dot(lhs[: 2 * height], t2, preferred_element_type=F32)
    y3 = jnp.dot(lhs[:height], t3, preferred_element_type=F32)
    h = height
    return y1[:h] + ((y1[h : 2 * h] + y2[:h]) + (y1[2 * h :] + y2[h : 2 * h] + y3))


def diagonal_tiles(parts_ref, sums_ref, tiles_ref, height, start, stop, offset=0):
    def step(index, carry):
        for u in range(UNROLL):
            t = index * UNROLL + u
            sums_ref[t] = tile_product(parts_ref, tiles_ref, t, t + offset, height)
        return carry

    lax.fori_loop(start // UNROLL, stop // UNROLL, step, 0)


def extra_tiles(parts_ref, sums_ref, tiles_ref, meta_ref, height, reach):
    row_tiles = sums_ref.shape[0]
    slots = tiles_ref.shape[1]
    base = meta_ref[0]
    count = meta_ref[2 * slots]

    def step(index, carry):
        found = []
        for u in range(UNROLL):
            t = row_tiles + index * UNROLL + u
            y = tile_product(parts_ref, tiles_ref, t, meta_ref[slots + t] - base + reach, height)
            found.append((meta_ref[t] - base, jnp.where(t < count, y, 0.0)))
        for row, y in found:
            sums_ref[row] += y
        return carry

    lax.fori_loop(0, (slots - row_tiles) // UNROLL, step, 0)


def split_kernel(tiles_ref, out_ref):
    def step(t, carry):
        for u in range(4):
            for k, part in enumerate(split3(tiles_ref[4 * t + u])):
                out_ref[k, 4 * t + u] = part
        return carry

    lax.fori_loop(0, tiles_ref.shape[0] // 4, step, 0)


def first_kernel(tile, meta_ref, x_ref, left_ref, right_ref, tiles_ref,
                 image_ref, first_ref, second_ref, parts_ref, sums_ref):
    channels = x_ref.shape[0]
    reach = left_ref.shape[1] // tile
    row_tiles = sums_ref.shape[0]
    odd = meta_ref[2 * tiles_ref.shape[1] + 1] == 1
    load_middle(parts_ref, reach, 0, channels, x_ref, tile)
    load_edges(parts_ref, 0, channels, left_ref.at[0:channels], right_ref.at[0:channels],
               row_tiles, tile, odd)
    diagonal_tiles(parts_ref, sums_ref, tiles_ref, channels, 0, row_tiles, reach)
    extra_tiles(parts_ref, sums_ref, tiles_ref, meta_ref, channels, reach)
    for i in range(row_tiles):
        cut = slice(i * tile, (i + 1) * tile)
        image_ref[:, cut] = x_ref[:, cut] - sums_ref[i]
    far = (row_tiles - reach) * tile
    head = image_ref[:, : reach * tile]
    tail = image_ref[:, far:]
    first_ref[...] = jnp.where(odd, head, tail)
    second_ref[...] = jnp.where(odd, tail, head)


def iota2(shape, dim):
    return lax.broadcasted_iota(jnp.int32, shape, dim)


def dot_nt(a, b):
    return lax.dot_general(a, b, (((1,), (1,)), ((), ())), precision=HIGHEST,
                           preferred_element_type=F32)


def middle_kernel(tile, x_ref, p_ref, ax_ref, tiles_ref,
                  sums_ref, basis_ref, quotient_ref, message_ref, parts_ref):
    k = x_ref.shape[0]
    load_middle(parts_ref, 0, 0, 2 * k, ax_ref, tile)
    load_middle(parts_ref, 0, k, 2 * k, p_ref, tile)
    diagonal_tiles(parts_ref, sums_ref, tiles_ref, 2 * k, 0, sums_ref.shape[0])
    x = x_ref[...]
    ax = ax_ref[...]
    q = jnp.sum(x * ax, axis=1, keepdims=True) / (jnp.sum(x * x, axis=1, keepdims=True) + 1e-06)
    basis_ref[0:k, :] = x
    basis_ref[k : 2 * k, :] = ax - q * x
    basis_ref[2 * k : 3 * k, :] = p_ref[...]
    basis_ref[3 * k : 4 * k, :] = ax
    quotient_ref[...] = jnp.broadcast_to(q, quotient_ref.shape)
    message_ref[...] = jnp.zeros_like(message_ref)
    message_ref[:, 0 : 4 * k] = dot_nt(basis_ref[0 : 3 * k, :], basis_ref[...])
    place = iota2((k, LANES), 1) == iota2((k, LANES), 0) + 6 * k
    message_ref[0:k, :] = jnp.where(place, q, message_ref[0:k, :])


def second_kernel(tile, meta_ref, p_ref, pleft_ref, pright_ref, ax_ref, aleft_ref, aright_ref,
                  tiles_ref, start_ref, basis_ref, quotient_ref, begun_ref,
                  a2x_ref, message_ref, parts_ref, sums_ref, images_ref):
    k = p_ref.shape[0]
    reach = aleft_ref.shape[1] // tile
    row_tiles = sums_ref.shape[0]
    odd = meta_ref[2 * tiles_ref.shape[1] + 1] == 1
    load_middle(parts_ref, reach, 0, 2 * k, ax_ref, tile)
    load_middle(parts_ref, reach, k, 2 * k, p_ref, tile)
    load_edges(parts_ref, k, 2 * k, pleft_ref.at[k : 2 * k], pright_ref.at[k : 2 * k],
               row_tiles, tile, odd)
    load_edges(parts_ref, 0, 2 * k, aleft_ref, aright_ref, row_tiles, tile, odd)
    sums_ref[...] = start_ref[...]
    extra_tiles(parts_ref, sums_ref, tiles_ref, meta_ref, 2 * k, reach)
    q = quotient_ref[:, 0:1]
    for i in range(row_tiles):
        cut = slice(i * tile, (i + 1) * tile)
        total = sums_ref[i]
        twice = ax_ref[:, cut] - total[:k]
        a2x_ref[:, cut] = twice
        images_ref[0:k, cut] = twice - q * ax_ref[:, cut]
        images_ref[k : 2 * k, cut] = p_ref[:, cut] - total[k:]
    message_ref[...] = begun_ref[...]
    message_ref[:, 4 * k : 6 * k] = dot_nt(basis_ref[0 : 3 * k, :], images_ref[...])


def tree(values):
    while len(values) > 1:
        values = [values[i] + values[i + 1] for i in range(0, len(values), 2)]
    return values[0]


def merged(messages, k):
    lane = iota2((k, LANES), 1)
    row = iota2((k, LANES), 0)
    squares, crosses, quotients = [], [], []
    for m in messages:
        top = m[0:k]
        squares.append(jnp.sum(jnp.where(lane == row, top, 0.0), axis=1, keepdims=True))
        crosses.append(jnp.sum(jnp.where(lane == row + 3 * k, top, 0.0), axis=1, keepdims=True))
        quotients.append(jnp.sum(jnp.where(lane == row + 6 * k, top, 0.0), axis=1, keepdims=True))
    q = tree(crosses) / (tree(squares) + 1e-06)
    lane_all = iota2((3 * k, LANES), 1)
    shifted = []
    for m, own in zip(messages, quotients):
        move = own - q
        m = jnp.where(lane_all < 6 * k, m, 0.0)
        m = jnp.concatenate([m[0:k], m[k : 2 * k] + move * m[0:k], m[2 * k :]], axis=0)
        picks = (lane == row) | (lane == row + 3 * k)
        across = jnp.sum(jnp.where(picks, move, 0.0), axis=0, keepdims=True)
        shifted.append(m + pltpu.roll(m * across, k, 1))
    return tree(shifted), q


def merge_kernel(*refs):
    *ins, out_ref = refs
    k = out_ref.shape[0] // 3
    total, q = merged([r[...] for r in ins], k)
    out_ref[...] = total
    place = iota2((k, LANES), 1) == iota2((k, LANES), 0) + 6 * k
    out_ref[0:k, :] = jnp.where(place, q, total[0:k])


def eliminate(matrix):
    n = matrix.shape[0]
    full = (8, LANES)
    blocks = [matrix[b : b + 8] for b in range(0, n, 8)]
    sub = iota2(full, 0)
    for g in range(0, n, GROUP):
        b0, r0 = divmod(g, 8)
        rows = [jnp.broadcast_to(blocks[b0][r0 + i : r0 + i + 1], full) for i in range(GROUP)]
        s = [[jnp.broadcast_to(rows[i][:, g + l : g + l + 1], full) if l >= i else None
              for l in range(GROUP)] for i in range(GROUP)]
        cols = {b: [jnp.broadcast_to(blocks[b][:, g + i : g + i + 1], full) for i in range(GROUP)]
                for b in range(b0, len(blocks))}
        for a in range(GROUP):
            inverse = 1.0 / s[a][a]
            for l in range(a + 1, GROUP):
                f = s[a][l] * inverse
                for c in range(l, GROUP):
                    s[l][c] = s[l][c] - f * s[a][c]
                rows[l] = rows[l] - f * rows[a]
                for b in cols:
                    cols[b][l] = cols[b][l] - f * cols[b][a]
            for b in cols:
                cols[b][a] = cols[b][a] * inverse
        for b in cols:
            update = blocks[b]
            for a in range(GROUP):
                update = update - cols[b][a] * rows[a]
            if b == b0:
                update = jnp.where(sub >= r0 + GROUP, update, blocks[b])
                for a in range(GROUP):
                    root = lax.rsqrt(s[a][a])
                    root = root * (1.5 - 0.5 * s[a][a] * root * root)
                    update = jnp.where(sub == r0 + a, rows[a] * root, update)
            blocks[b] = update
    return jnp.concatenate(blocks, axis=0)


def inverse_factor(gram):
    n = gram.shape[0]
    wide = jnp.concatenate([gram, jnp.zeros((n, LANES - n), F32)], axis=1)
    wide = jnp.where(iota2((n, LANES), 1) == iota2((n, LANES), 0) + n, 1.0, wide)
    done = eliminate(wide)
    return pltpu.roll(done, LANES - n, 1)[:, 0:n]


def dot_nn(a, b):
    return jnp.dot(a, b, precision=HIGHEST, preferred_element_type=F32)


def last_kernel(count, scale, locked_ref, *refs):
    messages = refs[:count]
    x_ref, ax_ref, a2x_ref, w_ref, wi_ref, ritz_ref = refs[count:]
    k = x_ref.shape[0]
    locked = locked_ref[0]
    total, q = merged([r[...] for r in messages], k)
    total = total * scale
    plain = total[:, 0 : 3 * k]
    image = pltpu.roll(total, LANES - 3 * k, 1)[:, 0 : 3 * k]
    row = iota2((k, k), 0)
    col = iota2((k, k), 1)
    active = (row >= locked) & (col >= locked)
    frozen = (row == col) & (row < locked)
    residual_gram = pltpu.roll(total, LANES - k, 1)[k : 2 * k, 0:k]
    gram_w = jnp.where(active, residual_gram, 0.0) + jnp.where(frozen, 1.0, 0.0)
    inverse_w = jnp.where(active, inverse_factor(gram_w), 0.0)
    residual = ax_ref[...] - q * x_ref[...]
    w_ref[...] = dot_nn(inverse_w, residual)
    wi_ref[...] = dot_nn(inverse_w, a2x_ref[...] - q * ax_ref[...])
    zeros = jnp.zeros((k, LANES - k), F32)
    mid = pltpu.roll(jnp.concatenate([inverse_w, zeros], axis=1), k, 1)[:, 0 : 3 * k]
    row3 = iota2((3 * k, 3 * k), 0)
    col3 = iota2((3 * k, 3 * k), 1)
    same = row3 == col3
    middle = (row3 >= k) & (row3 < 2 * k)
    empty = jnp.zeros((k, 3 * k), F32)
    change = jnp.where(same & ~middle, 1.0, jnp.concatenate([empty, mid, empty], axis=0))
    gram_b = dot_nt(dot_nn(change, plain), change)
    pad = same & (row3 >= k) & (row3 < k + locked)
    gram_b = gram_b + jnp.where(pad, 1.0, 0.0)
    gram_a = dot_nt(dot_nn(change, image), change)
    symmetric = 0.5 * (gram_a + gram_a.T)
    inverse_b = inverse_factor(gram_b)
    ritz_ref[...] = dot_nt(dot_nn(inverse_b, symmetric), inverse_b)


def stages(members):
    found, stride = [], 1
    while stride < members:
        size = 2
        found.append((stride, size))
        stride *= size
    assert stride == members
    return found


def body(current_block, previous_block, adjacency_tiles, tile_rows, tile_cols, tile_count, locked):
    k, rows_here = current_block.shape
    slots, tile, _ = adjacency_tiles.shape
    members = lax.axis_size(AXES)
    vertex_total = rows_here * members
    row_tiles = rows_here // tile
    reach = row_tiles // 2
    width = reach * tile
    span = row_tiles + 2 * reach
    inner = [(i, i ^ 1) for i in range(members)]
    outer = [(i, i + 1 if i % 2 else i - 1) for i in range(1, members - 1)]
    odd = lax.axis_index(AXES) % 2
    meta = jnp.concatenate([tile_rows, tile_cols, tile_count, odd[None].astype(jnp.int32)])

    def halo(first, second):
        return lax.ppermute(first, AXES, inner), lax.ppermute(second, AXES, outer)

    def sds(*shape):
        return jax.ShapeDtypeStruct(shape, F32)

    def edge(start):
        return jnp.concatenate(
            [
                lax.dynamic_slice_in_dim(block, start * (rows_here - width), width, 1)
                for block in (current_block, previous_block)
            ],
            axis=0,
        )

    left, right = halo(edge(1 - odd), edge(odd))
    params = pltpu.CompilerParams(vmem_limit_bytes=VMEM_LIMIT)
    cost = pl.CostEstimate(flops=10**8, bytes_accessed=10**7, transcendentals=0)
    parts = pl.pallas_call(
        split_kernel,
        out_shape=jax.ShapeDtypeStruct((3, slots, tile, tile), BF16),
        in_specs=[VMEM],
        out_specs=VMEM,
        compiler_params=params,
        cost_estimate=cost,
        name="split_tiles",
    )(adjacency_tiles)
    x_image, head, tail = pl.pallas_call(
        functools.partial(first_kernel, tile),
        out_shape=(sds(k, rows_here), sds(k, width), sds(k, width)),
        in_specs=[SMEM] + [VMEM] * 4,
        out_specs=(VMEM,) * 3,
        scratch_shapes=[
            pltpu.VMEM((span, 3 * k, tile), BF16),
            pltpu.VMEM((row_tiles, k, tile), F32),
        ],
        compiler_params=params,
        name="first_apply",
    )(meta, current_block, left, right, parts)
    aleft, aright = halo(head, tail)
    sums, basis, quotient, begun = pl.pallas_call(
        functools.partial(middle_kernel, tile),
        out_shape=(sds(row_tiles, 2 * k, tile), sds(4 * k, rows_here), sds(k, LANES),
                   sds(3 * k, LANES)),
        in_specs=[VMEM] * 4,
        out_specs=(VMEM,) * 4,
        scratch_shapes=[pltpu.VMEM((row_tiles, 6 * k, tile), BF16)],
        compiler_params=params,
        cost_estimate=cost,
        name="middle",
    )(current_block, previous_block, x_image, parts)
    twice, message = pl.pallas_call(
        functools.partial(second_kernel, tile),
        out_shape=(sds(k, rows_here), sds(3 * k, LANES)),
        in_specs=[SMEM] + [VMEM] * 11,
        out_specs=(VMEM,) * 2,
        scratch_shapes=[
            pltpu.VMEM((span, 6 * k, tile), BF16),
            pltpu.VMEM((row_tiles, 2 * k, tile), F32),
            pltpu.VMEM((2 * k, rows_here), F32),
        ],
        compiler_params=params,
        name="second_apply",
    )(meta, previous_block, left, right, x_image, aleft, aright, parts, sums, basis, quotient,
      begun)
    plan = stages(members)
    for number, (stride, size) in enumerate(plan):
        messages = [message] + [
            lax.ppermute(message, AXES, [(i, i ^ (m * stride)) for i in range(members)])
            for m in range(1, size)
        ]
        if number < len(plan) - 1:
            message = pl.pallas_call(
                merge_kernel,
                out_shape=sds(3 * k, LANES),
                in_specs=[VMEM] * size,
                out_specs=VMEM,
                compiler_params=pltpu.CompilerParams(vmem_limit_bytes=VMEM_LIMIT),
        name="merge",
            )(*messages)
    return pl.pallas_call(
        functools.partial(last_kernel, len(messages), 1.0 / vertex_total),
        out_shape=(sds(k, rows_here), sds(k, rows_here), sds(3 * k, 3 * k)),
        in_specs=[SMEM] + [VMEM] * (len(messages) + 3),
        out_specs=(VMEM,) * 3,
        compiler_params=pltpu.CompilerParams(vmem_limit_bytes=VMEM_LIMIT),
        name="finish",
    )(locked, *messages, current_block, x_image, twice)


def solution(mesh):
    in_specs = (
        P(None, ("graphs", "rows", "cols", "sub")),
        P(None, ("graphs", "rows", "cols", "sub")),
        P(("graphs", "rows", "cols", "sub"), None, None),
        P(("graphs", "rows", "cols", "sub")),
        P(("graphs", "rows", "cols", "sub")),
        P(("graphs", "rows", "cols", "sub")),
        P("graphs"),
    )
    out_specs = (
        P(None, ("graphs", "rows", "cols", "sub")),
        P(None, ("graphs", "rows", "cols", "sub")),
        P("graphs", None),
    )
    return jax.shard_map(body, mesh=mesh, in_specs=in_specs, out_specs=out_specs, check_vma=False)
```
